32 devices in a mesh: gx: 4 (over x, core), gy: 8 (over z, y).
Axes of the slice: x: 2, y: 2, z: 4, core: 2. Of those that a mesh axis runs over, the one named last changes fastest.
Arguments:
- midpoints: float32 [4, 8, 64, 3, 256], P('gx', 'gy'), may hold values from 0 to 1
- halves: float32 [4, 8, 64, 3, 256], P('gx', 'gy'), may hold values from -0.3 to 0.3
- burgers: float32 [4, 8, 64, 3, 256], P('gx', 'gy'), may hold values from -6 to 6
- mobility: float32 [4, 8, 64, 256], P('gx', 'gy'), may hold values from 0.5 to 2
- pair_left: int32 [4, 8, 128], P('gx', 'gy'), may hold values from 0 to 63
- pair_right: int32 [4, 8, 128], P('gx', 'gy'), may hold values from 0 to 63
- pair_slot: int32 [4, 8, 128], P('gx', 'gy'), may hold values from 0 to 4
- pair_count: int32 [4, 8], P('gx', 'gy'), may hold values from 1 to 128, as said below
Outputs:
- final_midpoints: float32 [4, 8, 64, 3, 256], P('gx', 'gy')
- corrector_force: float32 [4, 8, 64, 3, 256], P('gx', 'gy')
The draws below stay inside these ranges and needn't reach their ends.
Inputs may be any that keep to these rules, and one draw needn't show every extreme that they name: `pair_count`: slots at or beyond a device's count hold valid indices that are no pairs. In every draw some device has exactly 128 pairs.
All inputs are finite; a program needn't handle non-finite values.
Results may differ from the reference program's by a relative error of at most 0.0003.
Values sent between devices are 32-bit elements; how exact they have to be, the bound alone decides.
A program may use at most 128 MiB of HBM per device.

```python
import math
import jax
import jax.numpy as jnp
from jax import lax

BLOCK = 256
BLK_DEV = 64
PAIR_CAP = 128
N_GX = 4
N_GY = 8


def draw_pair_count(key, part):
    first_key, second_key = jax.random.split(jax.random.fold_in(key, 7))
    devices_all = N_GX * N_GY
    baseline = jax.random.randint(first_key, (devices_all,), 1, PAIR_CAP // 2 + 1)
    ranking = jax.random.permutation(second_key, devices_all)
    places = jnp.zeros((devices_all,), jnp.int32).at[ranking].set(jnp.arange(devices_all, dtype=jnp.int32))
    crowded = max(1, devices_all // 8)
    counts = jnp.where(places < crowded, PAIR_CAP, baseline)
    return counts.reshape((N_GX, N_GY)).astype(jnp.int32)


def plant(array, rng, smallest, high):
    extent = array.shape
    index_at = [jax.random.randint(jax.random.fold_in(rng, axis), (), 0, extent[axis]) for axis in range(len(extent))]
    array = array.at[tuple(index_at)].set(smallest)
    longest = extent.index(max(extent))
    index_at[longest] = (index_at[longest] + 1) % extent[longest]
    return array.at[tuple(index_at)].set(high)


def block_levels(stream_key, extent, shards, low, top_value):
    factor_of = 1.0
    for dim, shards_of in shards:
        draws = jax.random.uniform(jax.random.fold_in(jax.random.fold_in(stream_key, 6), dim), (shards_of,), jnp.float32, low / len(shards), top_value / len(shards))
        factor_of = factor_of * jnp.repeat(jnp.exp(draws), extent[dim] // shards_of).reshape((-1,) + (1,) * (len(extent) - 1 - dim))
    return factor_of


def noise(stream_key, extent, width, limit, cuts=(), held_as=jnp.bfloat16):
    array = jax.random.normal(stream_key, extent, jnp.float32) * width
    if len(cuts) > 0:
        array = block_levels(stream_key, extent, cuts, -0.22, 0.18) * array
    return jnp.clip(array, min=-limit, max=limit).astype(held_as)


def setup_inputs(seed: int = 0) -> dict:
    arg_keys = jax.random.split(jax.random.key(seed), 9)
    return {
        "midpoints": jnp.clip(1.0 * jax.random.uniform(arg_keys[0], (N_GX, N_GY, BLK_DEV, 3, BLOCK), jnp.float32) ** block_levels(arg_keys[0], (N_GX, N_GY, BLK_DEV, 3, BLOCK), ((0, 4), (1, 8)), -0.2, 0.2), 0.0, 1.0),
        "halves": noise(arg_keys[1], (N_GX, N_GY, BLK_DEV, 3, BLOCK), 0.05, 0.3, ((0, 4), (1, 8)), jnp.float32),
        "burgers": noise(arg_keys[2], (N_GX, N_GY, BLK_DEV, 3, BLOCK), 1.0, 6.0, ((0, 4), (1, 8)), jnp.float32),
        "mobility": jnp.clip(jnp.exp(math.log(2.0) - 1.3862944 * jax.random.uniform(arg_keys[3], (N_GX, N_GY, BLK_DEV, BLOCK), jnp.float32) ** block_levels(arg_keys[3], (N_GX, N_GY, BLK_DEV, BLOCK), ((0, 4), (1, 8)), -0.2, 0.2)), 0.5, 2.0),
        "pair_left": plant(jax.random.randint(arg_keys[4], (N_GX, N_GY, PAIR_CAP), 0, BLK_DEV), jax.random.fold_in(arg_keys[4], 1), 0, BLK_DEV - 1).astype(jnp.int32),
        "pair_right": plant(jax.random.randint(arg_keys[5], (N_GX, N_GY, PAIR_CAP), 0, BLK_DEV), jax.random.fold_in(arg_keys[5], 1), 0, BLK_DEV - 1).astype(jnp.int32),
        "pair_slot": plant(jax.random.randint(arg_keys[6], (N_GX, N_GY, PAIR_CAP), 0, 5), jax.random.fold_in(arg_keys[6], 1), 0, 4).astype(jnp.int32),
        "pair_count": draw_pair_count(jax.random.fold_in(arg_keys[8], 71), 0),
    }


core_square = 0.04
poisson_part = 0.6
time_step = 0.1
gauss_offset = 0.5773502691896258

def pair_forces(mid_a, half_a, burg_a, mid_b, half_b, burg_b, offset):
    burg_dot = jnp.einsum('...ci,...cj->...ij', burg_a, burg_b, precision=lax.Precision.HIGHEST)
    half_dot = jnp.einsum('...ci,...cj->...ij', half_a, half_b, precision=lax.Precision.HIGHEST)
    screw_a = lax.optimization_barrier(jnp.sum(burg_a * half_a, axis=-2))
    screw_b = lax.optimization_barrier(jnp.sum(burg_b * half_b, axis=-2))
    coupling = 4.0 * (burg_dot * half_dot + poisson_part * screw_a[..., :, None] * screw_b[..., None, :])
    force_a = jnp.zeros_like(mid_a)
    force_b = jnp.zeros_like(mid_b)
    for sign_a in (1.0, -1.0):
        for sign_b in (1.0, -1.0):
            point_a = mid_a + sign_a * gauss_offset * half_a
            point_b = mid_b + offset + sign_b * gauss_offset * half_b
            pieces = [point_a[..., component, :, None] - point_b[..., component, None, :] for component in range(3)]
            distance = core_square + pieces[0] * pieces[0] + pieces[1] * pieces[1] + pieces[2] * pieces[2]
            inverse = 1.0 / jnp.sqrt(distance)
            kernel = 0.25 * coupling * inverse * inverse * inverse * (1.0 + 1.5 * core_square * inverse * inverse)
            force_a = force_a + jnp.stack([lax.optimization_barrier(jnp.sum(kernel * piece, axis=-1)) for piece in pieces], axis=-2)
            force_b = force_b - jnp.stack([lax.optimization_barrier(jnp.sum(kernel * piece, axis=-2)) for piece in pieces], axis=-2)
    return (force_a, force_b)

def reference(midpoints, halves, burgers, mobility, pair_left, pair_right, pair_slot, pair_count):
    fixed_parts = jnp.concatenate([halves, burgers], axis=3)

    def evaluate(middles):
        blocks = jnp.concatenate([middles, fixed_parts], axis=3)

        def device(number, forces_sum):
            cell_x = number // N_GY
            cell_y = number % N_GY

            def one_pair(pair_id, running):
                left_id = pair_left[cell_x, cell_y, pair_id]
                right_id = pair_right[cell_x, cell_y, pair_id]
                slot_id = pair_slot[cell_x, cell_y, pair_id]
                shift_x = jnp.where((slot_id == 1) | (slot_id == 3) | (slot_id == 4), 1, 0)
                shift_y = jnp.where((slot_id == 2) | (slot_id == 3), 1, jnp.where(slot_id == 4, -1, 0))
                other_x = (cell_x + shift_x) % N_GX
                other_y = (cell_y + shift_y) % N_GY
                first_rows = blocks[cell_x, cell_y, left_id]
                second_rows = blocks[other_x, other_y, right_id]
                offset = jnp.stack([shift_x, shift_y, 0 * shift_x]).astype(jnp.float32)[:, None]
                force_a, force_b = pair_forces(first_rows[:3], first_rows[3:6], first_rows[6:], second_rows[:3], second_rows[3:6], second_rows[6:], offset)
                reverse = jnp.where((slot_id == 0) & (left_id == right_id), 0.0, 1.0)
                running = running.at[cell_x, cell_y, left_id].add(force_a)
                return running.at[other_x, other_y, right_id].add(reverse * force_b)
            return lax.fori_loop(0, pair_count[cell_x, cell_y], one_pair, forces_sum)
        return lax.fori_loop(0, N_GX * N_GY, device, jnp.zeros_like(middles))
    force_one = evaluate(midpoints)
    moved = midpoints + time_step * mobility[:, :, :, None, :] * force_one
    force_two = evaluate(moved)
    final_midpoints = midpoints + 0.5 * time_step * mobility[:, :, :, None, :] * (force_one + force_two)
    return (final_midpoints, force_two)
```

```python
import jax
import jax.numpy as jnp
from jax import lax
from jax.experimental import pallas as pl
from jax.experimental.pallas import tpu as pltpu
from jax.sharding import PartitionSpec as P

core_square = 0.04
poisson_part = 0.6
time_step = 0.1
gauss_offset = 0.5773502691896258
length_square = 1.5 * core_square
to_scaled = length_square**-0.5


def from_behind(x, axis, by):
    devices = lax.axis_size(axis)
    return lax.ppermute(x, axis, [(i, (i + by) % devices) for i in range(devices)])


def split_three(x):
    high = x.astype(jnp.bfloat16).astype(jnp.float32)
    rest = x - high
    middle = rest.astype(jnp.bfloat16).astype(jnp.float32)
    return high, middle, rest - middle


def prepare(k, ids, mid_ref, fixed_ref, buffers):
    cross_ref, couple_ref, column_ref, row_ref = buffers
    left_ref, right_ref, slot_ref = ids
    blocks = mid_ref.shape[0] // 5
    segments = mid_ref.shape[2]
    left = left_ref[k]
    kind = slot_ref[k]
    right = kind * blocks + right_ref[k]
    east = jnp.where((kind == 1) | (kind >= 3), 1.0, 0.0).astype(jnp.float32)
    north = jnp.where(
        (kind == 2) | (kind == 3), 1.0, jnp.where(kind == 4, -1.0, 0.0)
    ).astype(jnp.float32)
    component = lax.broadcasted_iota(jnp.int32, (3, segments), 0)
    offset = jnp.where(component == 0, east, jnp.where(component == 1, north, 0.0))
    mid_a = mid_ref[left] * to_scaled
    mid_b = (mid_ref[right] + offset) * to_scaled
    fixed_a = fixed_ref[left]
    fixed_b = fixed_ref[right]
    half_a, burg_a = fixed_a[:3], fixed_a[3:]
    half_b, burg_b = fixed_b[:3], fixed_b[3:]
    arm_a = half_a * (gauss_offset * to_scaled)
    arm_b = half_b * (gauss_offset * to_scaled)

    ones = jnp.ones((1, segments), jnp.float32)
    arm_square_a = jnp.sum(arm_a * arm_a, axis=0, keepdims=True)
    arm_square_b = jnp.sum(arm_b * arm_b, axis=0, keepdims=True)
    tilt_a = 2.0 * jnp.sum(mid_a * arm_a, axis=0, keepdims=True)
    tilt_b = 2.0 * jnp.sum(mid_b * arm_b, axis=0, keepdims=True)
    base_b = arm_square_b + core_square / length_square
    form_a = jnp.concatenate(
        [
            jnp.concatenate([-2.0 * arm_a, mid_a, arm_square_a + tilt_a, ones], axis=0),
            jnp.concatenate([2.0 * arm_a, mid_a, arm_square_a - tilt_a, ones], axis=0),
        ],
        axis=1,
    )
    form_b = jnp.concatenate(
        [
            jnp.concatenate([mid_b + arm_b, -2.0 * arm_b, ones, base_b + tilt_b], axis=0),
            jnp.concatenate([mid_b - arm_b, 2.0 * arm_b, ones, base_b - tilt_b], axis=0),
        ],
        axis=1,
    )
    high_a, middle_a, low_a = split_three(form_a)
    high_b, middle_b, low_b = split_three(form_b)
    wide_a = jnp.concatenate([high_a, high_a, middle_a, high_a, low_a, middle_a], axis=0)
    wide_b = jnp.concatenate([high_b, middle_b, high_b, low_b, high_b, middle_b], axis=0)
    cross_ref[...] = jnp.dot(
        jnp.transpose(wide_a).astype(jnp.bfloat16),
        wide_b.astype(jnp.bfloat16),
        preferred_element_type=jnp.float32,
    )

    screw_a = jnp.sum(burg_a * half_a, axis=0, keepdims=True) * poisson_part
    screw_b = jnp.sum(burg_b * half_b, axis=0, keepdims=True)
    blank = jnp.zeros((6, segments), jnp.float32)
    pair_a = jnp.concatenate(
        [burg_a[:1] * half_a, burg_a[1:2] * half_a, burg_a[2:] * half_a, screw_a, blank], axis=0
    )
    pair_b = jnp.concatenate(
        [burg_b[:1] * half_b, burg_b[1:2] * half_b, burg_b[2:] * half_b, screw_b, blank], axis=0
    ) * (1.0 / length_square)
    top_a = pair_a.astype(jnp.bfloat16).astype(jnp.float32)
    top_b = pair_b.astype(jnp.bfloat16).astype(jnp.float32)
    couple_ref[...] = jnp.dot(
        jnp.transpose(jnp.concatenate([top_a, top_a, pair_a - top_a], axis=0)).astype(jnp.bfloat16),
        jnp.concatenate([top_b, pair_b - top_b, top_b], axis=0).astype(jnp.bfloat16),
        preferred_element_type=jnp.float32,
    )
    spare = jnp.zeros((2, segments), jnp.float32)
    column_ref[...] = jnp.transpose(jnp.concatenate([mid_a, arm_a, spare], axis=0))
    row_ref[...] = jnp.concatenate([mid_b, arm_b, spare], axis=0)


def interact(k, live, ids, buffers, sum_ref, force_ref):
    cross_ref, couple_ref, column_ref, row_ref = buffers
    left_ref, right_ref, slot_ref = ids
    blocks = force_ref.shape[0] // 5
    segments = row_ref.shape[1]
    total_b = [jnp.zeros((8, segments), jnp.float32) for _ in range(3)]
    for top in range(0, segments, 8):
        gaps = [
            column_ref[top : top + 8, c : c + 1] - row_ref[c : c + 1, :] for c in range(3)
        ]
        square = gaps[0] * gaps[0] + gaps[1] * gaps[1] + gaps[2] * gaps[2]
        weights = []
        for start in (top, segments + top):
            for column in (0, segments):
                y = square + cross_ref[start : start + 8, column : column + segments]
                inverse = lax.rsqrt(y)
                inverse_square = inverse * inverse
                weights.append((inverse * inverse_square) * (1.0 + inverse_square))
        same_sum = weights[0] + weights[3]
        cross_sum = weights[1] + weights[2]
        same_gap = weights[0] - weights[3]
        cross_gap = weights[1] - weights[2]
        couple = couple_ref[top : top + 8, :]
        whole = couple * (same_sum + cross_sum)
        along_a = couple * (same_gap + cross_gap)
        along_b = couple * (same_gap - cross_gap)
        for c in range(3):
            force = (
                whole * gaps[c]
                + along_a * column_ref[top : top + 8, 3 + c : 4 + c]
                - along_b * row_ref[3 + c : 4 + c, :]
            )
            total_b[c] = total_b[c] + force
            folded = force[:, :128]
            for lane in range(128, segments, 128):
                folded = folded + force[:, lane : lane + 128]
            sum_ref[c * segments + top : c * segments + top + 8, :] = folded
    force_a = jnp.concatenate(
        [
            jnp.concatenate(
                [
                    jnp.sum(
                        jnp.transpose(
                            sum_ref[c * segments + lane : c * segments + lane + 128, :]
                        ),
                        axis=0,
                        keepdims=True,
                    )
                    for lane in range(0, segments, 128)
                ],
                axis=1,
            )
            for c in range(3)
        ],
        axis=0,
    )
    force_b = jnp.concatenate([jnp.sum(t, axis=0, keepdims=True) for t in total_b], axis=0)
    left = left_ref[k]
    kind = slot_ref[k]
    right = kind * blocks + right_ref[k]
    active = k < live
    force_ref[left] = force_ref[left] + jnp.where(active, force_a, 0.0)
    mutual = active & (left != right)
    force_ref[right] = force_ref[right] - jnp.where(mutual, force_b, 0.0)


def sweep_body(
    count_ref, left_ref, right_ref, slot_ref, mid_ref, fixed_ref, force_ref, *scratch
):
    even, odd = scratch[:4], scratch[4:8]
    even_sum, odd_sum = scratch[8:]
    ids = (left_ref, right_ref, slot_ref)
    live = count_ref[0]
    last = left_ref.shape[0] - 1
    force_ref[...] = jnp.zeros_like(force_ref)
    prepare(0, ids, mid_ref, fixed_ref, even)

    def advance(step, carry):
        first = 2 * step
        second = jnp.minimum(first + 1, last)
        third = jnp.minimum(first + 2, last)
        prepare(second, ids, mid_ref, fixed_ref, odd)
        interact(first, live, ids, even, even_sum, force_ref)
        prepare(third, ids, mid_ref, fixed_ref, even)
        live_second = jnp.where(first + 1 < live, live, 0)
        interact(second, live_second, ids, odd, odd_sum, force_ref)
        return carry

    lax.fori_loop(0, (live + 1) // 2, advance, 0)


def sweep(near_mids, near_fixed, left_rows, right_rows, slot_rows, live_count):
    segments = near_mids.shape[2]
    buffers = [
        pltpu.VMEM((2 * segments, 2 * segments), jnp.float32),
        pltpu.VMEM((segments, segments), jnp.float32),
        pltpu.VMEM((segments, 8), jnp.float32),
        pltpu.VMEM((8, segments), jnp.float32),
    ]
    sums = pltpu.VMEM((3 * segments, 128), jnp.float32)
    scalar = pl.BlockSpec(memory_space=pltpu.SMEM)
    vector = pl.BlockSpec(memory_space=pltpu.VMEM)
    return pl.pallas_call(
        sweep_body,
        name="pair_sweep",
        out_shape=jax.ShapeDtypeStruct(near_mids.shape, jnp.float32),
        in_specs=[scalar] * 4 + [vector] * 2,
        out_specs=vector,
        scratch_shapes=buffers + buffers + [sums, sums],
        compiler_params=pltpu.CompilerParams(vmem_limit_bytes=48 * 1024 * 1024),
    )(live_count, left_rows, right_rows, slot_rows, near_mids, near_fixed)


def gather_near(blocks):
    eastern = from_behind(blocks, "gx", -1)
    northern = from_behind(blocks, "gy", -1)
    north_east = from_behind(eastern, "gy", -1)
    south_east = from_behind(eastern, "gy", 1)
    return jnp.concatenate([blocks, eastern, northern, north_east, south_east])


def give_back(forces):
    own, eastern, northern, north_east, south_east = jnp.split(forces, 5)
    eastern = eastern + from_behind(north_east, "gy", 1) + from_behind(south_east, "gy", -1)
    return own + from_behind(northern, "gy", 1) + from_behind(eastern, "gx", 1)


def on_device(midpoints, halves, burgers, mobility, pair_left, pair_right, pair_slot, pair_count):
    middles = midpoints[0, 0]
    mobile = mobility[0, 0][:, None, :]
    pairs = (pair_left[0, 0], pair_right[0, 0], pair_slot[0, 0], pair_count[0])
    near_fixed = gather_near(jnp.concatenate([halves[0, 0], burgers[0, 0]], axis=1))
    near_mids = gather_near(middles)
    force_one = give_back(sweep(near_mids, near_fixed, *pairs))
    moved = middles + time_step * mobile * force_one
    force_two = give_back(sweep(gather_near(moved), near_fixed, *pairs))
    final_midpoints = middles + 0.5 * time_step * mobile * (force_one + force_two)
    return (final_midpoints[None, None], force_two[None, None])


def solution(mesh):
    return jax.shard_map(
        on_device,
        mesh=mesh,
        in_specs=(
            P("gx", "gy", None, None, None),
            P("gx", "gy", None, None, None),
            P("gx", "gy", None, None, None),
            P("gx", "gy", None, None),
            P("gx", "gy", None),
            P("gx", "gy", None),
            P("gx", "gy", None),
            P("gx", "gy"),
        ),
        out_specs=(P("gx", "gy", None, None, None), P("gx", "gy", None, None, None)),
        check_vma=False,
    )
```
